256 devices in a mesh: tm: 64 (over z, y_lo, x), space: 4 (over y_hi, core).
Axes of the slice: x: 4, y: 4 (y_hi: 2, y_lo: 2; y = y_hi * 2 + y_lo), z: 8, core: 2. Of those that a mesh axis runs over, the one named last changes fastest.
Arguments:
- checkpoint: float32 [64, 4, 64, 1024], P('tm', None, 'space'), may hold values from -6 to 6
- advect: float32 [64, 2, 64, 1024], P('tm', None, 'space'), may hold values from -0.2 to 0.2
- diffuse: float32 [64, 64, 1024], P('tm', 'space'), may hold values from 0.1 to 0.2
- obs_rows: int32 [64, 8, 8], P('tm', None, 'space'), may hold values from 0 to 1
- obs_values: float32 [64, 8, 8, 4, 8, 1024], P('tm', None, 'space'), may hold values from -6 to 6
- obs_weight: float32 [64], P('tm'), may hold values from 0.5 to 13.5
- error_inverse: float32 [64, 4], P('tm'), may hold values from 0.3 to 3
- rates: float32 [64, 4], replicated, may hold values from 0.3971641 to 1, as said below
Outputs:
- direction: float32 [64, 4, 64, 1024], P('tm', None, 'space')
- grad_rms: float32 [], replicated
The draws below stay inside these ranges and needn't reach their ends.
Inputs may be any that keep to these rules, and one draw needn't show every extreme that they name: `obs_rows`: entry i of the last dimension counts blocks of 8 rows within the rows of space block i // 2; repeats may occur. `rates`: every entry is below 1.
All inputs are finite; a program needn't handle non-finite values.
Results may differ from the reference program's by a relative error of at most 0.0003.
Values sent between devices are 32-bit elements; how exact they have to be, the bound alone decides.
No kernel may reach another device: no remote copies, remote signals or barrier semaphores. Data moves between devices by JAX's collectives and lax.ppermute only.
A program may use at most 64 MiB of HBM per device.

```python
import math
import jax
import jax.numpy as jnp
from jax import lax

STATE_COMPONENTS = 4
NX = 1024
ROWS = 16
STEPS = 8
BLOCK = 8
KOBS = 2
SUBWINDOW_COUNT = 64
NY = 64
NOBS = 8


def draw_obs_weight(key, part):
    places = jnp.arange(SUBWINDOW_COUNT, dtype=jnp.float32) / max(SUBWINDOW_COUNT - 1, 1)
    rising = 3.0 ** places
    jitter = jax.random.uniform(key, (SUBWINDOW_COUNT,), jnp.float32, 0.8, 1.2)
    return rising * jitter


def draw_rates(key, part):
    random_key_parts = jax.random.split(jax.random.fold_in(key, 7), 5)
    slow_share = 0.5
    is_slow = jax.random.uniform(random_key_parts[0], (STATE_COMPONENTS,), jnp.float32) < slow_share
    slow_strength = jax.random.uniform(random_key_parts[1], (STATE_COMPONENTS,), jnp.float32, 0.15, 0.4)
    fast_strength = jax.random.uniform(random_key_parts[1], (STATE_COMPONENTS,), jnp.float32, 2.0, 4.0)
    strength = jnp.where(is_slow, slow_strength, fast_strength)
    factor = jnp.exp(jax.random.uniform(random_key_parts[2], (SUBWINDOW_COUNT, STATE_COMPONENTS), jnp.float32, jnp.log(0.6), jnp.log(1.6)))
    logarithm_rate = jnp.log(0.1) * strength[None, :] * factor / SUBWINDOW_COUNT
    surge_location = jax.random.randint(random_key_parts[3], (2, STATE_COMPONENTS), 0, SUBWINDOW_COUNT)
    inside_surge = jnp.any(jnp.arange(SUBWINDOW_COUNT)[:, None, None] == surge_location[None, :, :], axis=1)
    reduction_factor = jax.random.uniform(random_key_parts[4], (SUBWINDOW_COUNT, STATE_COMPONENTS), jnp.float32, 0.5, 0.8)
    return jnp.exp(logarithm_rate) * jnp.where(inside_surge, reduction_factor, 1.0)


def with_ends(entries, stream_key, smallest, largest):
    longest = entries.shape.index(max(entries.shape))
    spots = []
    for shift in (0, 1):
        where = [jax.random.randint(jax.random.fold_in(stream_key, axis), (), 0, length) for axis, length in enumerate(entries.shape)]
        where[longest] = (where[longest] + shift) % entries.shape[longest]
        spots.append(tuple(where))
    return entries.at[spots[0]].set(smallest).at[spots[1]].set(largest)


def steps_of(key, shape, cuts, smallest, largest):
    gain = 1.0
    for position, parts in cuts:
        heights = jax.random.uniform(jax.random.fold_in(jax.random.fold_in(key, 6), position), (parts,), jnp.float32, smallest / len(cuts), largest / len(cuts))
        gain = gain * jnp.repeat(jnp.exp(heights), shape[position] // parts).reshape((-1,) + (1,) * (len(shape) - 1 - position))
    return gain


def gaussian(stream_key, dims, deviation, limit, cuts=(), held_as=jnp.bfloat16):
    drawn = jax.random.normal(stream_key, dims, jnp.float32) * deviation
    if len(cuts) > 0:
        drawn = steps_of(stream_key, dims, cuts, -0.22, 0.18) * drawn
    return jnp.clip(drawn, min=-limit, max=limit).astype(held_as)


def setup_inputs(seed: int = 0) -> dict:
    keys = jax.random.split(jax.random.key(seed), 9)
    checkpoint = gaussian(keys[0], (SUBWINDOW_COUNT, STATE_COMPONENTS, NY, NX), 1.0, 6.0, ((0, 64), (2, 4)), jnp.float32)
    advect = jnp.clip(jax.random.uniform(keys[1], (SUBWINDOW_COUNT, 2, NY, NX), jnp.float32, -0.2, 0.2) * steps_of(keys[1], (SUBWINDOW_COUNT, 2, NY, NX), ((0, 64), (2, 4)), -0.4, 0.0), -0.2, 0.2)
    diffuse = jnp.clip(0.1 + 0.1 * jax.random.uniform(keys[2], (SUBWINDOW_COUNT, NY, NX), jnp.float32) ** steps_of(keys[2], (SUBWINDOW_COUNT, NY, NX), ((0, 64), (1, 4)), -0.2, 0.2), 0.1, 0.2)
    obs_rows = with_ends(jax.random.randint(keys[3], (SUBWINDOW_COUNT, STEPS, NOBS), 0, ROWS // BLOCK), jax.random.fold_in(keys[3], 1), 0, (ROWS // BLOCK) - 1).astype(jnp.int32)
    obs_values = gaussian(keys[4], (SUBWINDOW_COUNT, STEPS, NOBS, STATE_COMPONENTS, BLOCK, NX), 1.0, 6.0, ((0, 64), (2, 4)), jnp.float32)
    obs_weight = draw_obs_weight(jax.random.fold_in(keys[8], 71), 0)
    error_inverse = jnp.clip(jnp.exp(math.log(3.0) - 2.3025851 * jax.random.uniform(keys[6], (SUBWINDOW_COUNT, STATE_COMPONENTS), jnp.float32) ** steps_of(keys[6], (SUBWINDOW_COUNT, STATE_COMPONENTS), ((0, 64),), -0.2, 0.2)), 0.3, 3.0)
    rates = draw_rates(jax.random.fold_in(keys[8], 71), 0)
    return {"checkpoint": checkpoint, "advect": advect, "diffuse": diffuse, "obs_rows": obs_rows, "obs_values": obs_values, "obs_weight": obs_weight, "error_inverse": error_inverse, "rates": rates}


def weights_of(advect_one, diffuse_one):
    centre = 1.0 - 4.0 * diffuse_one
    to_east = diffuse_one - 0.5 * advect_one[0]
    to_west = diffuse_one + 0.5 * advect_one[0]
    to_north = diffuse_one - 0.5 * advect_one[1]
    to_south = diffuse_one + 0.5 * advect_one[1]
    return (centre, to_east, to_west, to_north, to_south)

def pad_rows(values_in):
    return jnp.pad(values_in, ((0, 0), (1, 1), (0, 0)))

def advance(field_now, stencil):
    centre, to_east, to_west, to_north, to_south = stencil
    padded = pad_rows(field_now)
    return centre * field_now + to_east * jnp.roll(field_now, -1, axis=2) + to_west * jnp.roll(field_now, 1, axis=2) + to_north * padded[:, 2:] + to_south * padded[:, :-2]

def retreat(costate, stencil):
    centre, to_east, to_west, to_north, to_south = stencil
    north_flux = pad_rows(to_north * costate)
    south_flux = pad_rows(to_south * costate)
    return centre * costate + jnp.roll(to_east * costate, 1, axis=2) + jnp.roll(to_west * costate, -1, axis=2) + north_flux[:, :-2] + south_flux[:, 2:]

def row_index(rows_step):
    first_rows = jnp.arange(NOBS, dtype=jnp.int32) // KOBS * ROWS + rows_step.astype(jnp.int32) * BLOCK
    return first_rows[:, None] + jnp.arange(BLOCK, dtype=jnp.int32)[None, :]

def observe(field_now, row_picks):
    return jnp.transpose(field_now[:, row_picks], (1, 0, 2, 3))

def spread(misfit, row_picks):
    empty_field = jnp.zeros((STATE_COMPONENTS, NY, NX), jnp.float32)
    return empty_field.at[:, row_picks].add(jnp.transpose(misfit, (1, 0, 2, 3)))

def sweep_forward(packed):
    initial, advect_one, diffuse_one, rows_one, values_one = packed
    stencil = weights_of(advect_one, diffuse_one)
    field_now = initial
    misfits = []
    for moment in range(STEPS):
        field_now = advance(field_now, stencil)
        misfits.append(observe(field_now, row_index(rows_one[moment])) - values_one[moment])
    return (field_now, jnp.stack(misfits))

def sweep_back(packed):
    advect_one, diffuse_one, rows_one, misfit_one, obs_scale, next_term, own_term = packed
    stencil = weights_of(advect_one, diffuse_one)
    costate = spread(obs_scale * misfit_one[STEPS - 1], row_index(rows_one[STEPS - 1])) - next_term
    for moment in range(STEPS, 0, -1):
        costate = retreat(costate, stencil)
        if moment >= 2:
            costate = costate + spread(obs_scale * misfit_one[moment - 2], row_index(rows_one[moment - 2]))
    return costate + own_term

def forward_carry(running, packed):
    rate_row, inno_row, grad_one = packed
    updated = rate_row[:, None, None] * running + inno_row[:, None, None] * grad_one
    return (updated, updated)

def backward_carry(running, packed):
    rate_row, inno_row, forward_one = packed
    updated = inno_row[:, None, None] * forward_one + rate_row[:, None, None] * running
    return (updated, updated)

def reference(checkpoint, advect, diffuse, obs_rows, obs_values, obs_weight, error_inverse, rates):
    end_states, misfits = lax.map(sweep_forward, (checkpoint, advect, diffuse, obs_rows, obs_values))
    prior_end = jnp.concatenate([jnp.zeros_like(end_states[:1]), end_states[:-1]], axis=0)
    forcing = checkpoint - prior_end
    weighted = error_inverse[:, :, None, None] * forcing
    next_term = jnp.concatenate([weighted[1:], jnp.zeros_like(weighted[:1])], axis=0)
    gradient = lax.map(sweep_back, (advect, diffuse, obs_rows, misfits, obs_weight, next_term, weighted))
    square_sum = jnp.sum(gradient * gradient)
    rms_value = jnp.sqrt(square_sum / (SUBWINDOW_COUNT * STATE_COMPONENTS * NY * NX) + 1e-06)
    innovation = jnp.sqrt(1.0 - rates * rates)
    next_rates = jnp.concatenate([rates[1:], jnp.zeros((1, STATE_COMPONENTS), jnp.float32)], axis=0)
    zero_field = jnp.zeros((STATE_COMPONENTS, NY, NX), jnp.float32)
    _, smoothed = lax.scan(forward_carry, zero_field, (rates, innovation, gradient))
    _, result = lax.scan(backward_carry, zero_field, (next_rates, innovation, smoothed), reverse=True)
    return (result / rms_value, rms_value)
```

```python
import jax
import jax.numpy as jnp
from jax import lax
from jax.experimental import pallas as pl
from jax.experimental.pallas import tpu as pltpu
from jax.sharding import Mesh
from jax.sharding import PartitionSpec as P

STEPS = 8
BLOCK = 8
COMPS = 4
ROWS = 16
LANES = 128
GROUPS = 8
COLUMNS = GROUPS * LANES
TALL = 48
FIRST = 8
OWN = 16
CELLS = COMPS * GROUPS
SPACE = ("space_0", "space_1")
TM = ("tm_0", "tm_1", "tm_2")
VMEM = pl.BlockSpec(memory_space=pltpu.VMEM)
SMEM = pl.BlockSpec(memory_space=pltpu.SMEM)
ANY = pl.BlockSpec(memory_space=pl.ANY)


def shape(*dims):
    return jax.ShapeDtypeStruct(dims, jnp.float32)


def lanes(group):
    return slice(group * LANES, (group + 1) * LANES)


def passed_along(value, axis, steps):
    count = lax.axis_size(axis)
    leading, last = (max(0, -steps), min(count, count - steps))
    return lax.ppermute(value, axis, [(source, source + steps) for source in range(leading, last)])


def swapped(value, axis):
    return lax.ppermute(value, axis, [(0, 1), (1, 0)])


def eastern(tiles, lane):
    turned = [pltpu.roll(tile, LANES - 1, 1) for tile in tiles]
    return [
        jnp.where(lane == LANES - 1, turned[(g + 1) % GROUPS], turned[g]) for g in range(GROUPS)
    ]


def western(tiles, lane):
    turned = [pltpu.roll(tile, 1, 1) for tile in tiles]
    return [jnp.where(lane == 0, turned[g - 1], turned[g]) for g in range(GROUPS)]


def coefficient_tiles(advect, diffuse, low, high, tile, group):
    if tile in (1, 2):
        rows = slice((tile - 1) * 8, tile * 8)
        east_flow = advect[0, rows, lanes(group)]
        north_flow = advect[1, rows, lanes(group)]
        spread = diffuse[rows, lanes(group)]
    else:
        side = low if tile == 0 else high
        east_flow = side[32:40, lanes(group)]
        north_flow = side[40:48, lanes(group)]
        spread = side[48:56, lanes(group)]
    return (
        1.0 - 4.0 * spread,
        spread - 0.5 * east_flow,
        spread + 0.5 * east_flow,
        spread - 0.5 * north_flow,
        spread + 0.5 * north_flow,
    )


def lane_index():
    return lax.broadcasted_iota(jnp.int32, (8, LANES), 1)


def stencil_tile(source, tile, lane, centre, east, west, north, south, store):
    fields = [[source(k, g, 0) for g in range(GROUPS)] for k in range(COMPS)]
    to_east = [eastern(row, lane) for row in fields]
    to_west = [western(row, lane) for row in fields]
    for g in range(GROUPS):
        c, e, w, n, s = centre(g), east(g), west(g), north(g), south(g)
        for k in range(COMPS):
            store(
                k,
                g,
                c * fields[k][g]
                + e * to_east[k][g]
                + w * to_west[k][g]
                + n * source(k, g, 1)
                + s * source(k, g, -1),
            )


def forward_kernel(checkpoint, advect, diffuse, low, high, history, last, coefs, work):
    lane = lane_index()
    nothing = jnp.zeros((8, LANES), jnp.float32)
    for g in range(GROUPS):
        for tile in range(4):
            rows = slice(FIRST + 8 * tile, FIRST + 8 * tile + 8)
            values = coefficient_tiles(advect, diffuse, low, high, tile, g)
            for which in range(5):
                coefs[which, g, rows, :] = values[which]
            for k in range(COMPS):
                if tile in (1, 2):
                    value = checkpoint[k, (tile - 1) * 8 : tile * 8, lanes(g)]
                else:
                    value = (low if tile == 0 else high)[8 * k : 8 * k + 8, lanes(g)]
                work[0, k * GROUPS + g, rows, :] = value
        for k in range(COMPS):
            for slot in range(2):
                work[slot, k * GROUPS + g, 0:8, :] = nothing
                work[slot, k * GROUPS + g, TALL - 8 : TALL, :] = nothing

    def step(moment, carry):
        now = lax.rem(moment, 2)
        after = 1 - now
        for tile in range(4):
            start = FIRST + 8 * tile

            def source(k, g, shift):
                return work[now, k * GROUPS + g, start + shift : start + shift + 8, :]

            def store(k, g, value):
                work[after, k * GROUPS + g, start : start + 8, :] = value
                if tile in (1, 2):
                    history[moment, k * GROUPS + g, (tile - 1) * 8 : tile * 8, :] = value

            loads = [
                lambda g, which=which: coefs[which, g, start : start + 8, :] for which in range(5)
            ]
            stencil_tile(source, tile, lane, *loads, store)
        return carry

    lax.fori_loop(0, STEPS, step, 0)
    for cell in range(CELLS):
        last[cell] = history[STEPS - 1, cell]


def adjoint_kernel(
    obs_rows, weight, advect, diffuse, low, high, history, following, obs_values,
    own, to_low, to_high, coefs, work, observed, arrivals,
):
    copies = [
        pltpu.make_async_copy(obs_values.at[moment], observed.at[moment], arrivals.at[moment])
        for moment in range(STEPS)
    ]
    for moment in reversed(range(STEPS)):
        copies[moment].start()
    lane = lane_index()
    nothing = jnp.zeros((8, LANES), jnp.float32)
    for tile in range(4):
        rows = slice(FIRST + 8 * tile, FIRST + 8 * tile + 8)
        groups = [
            coefficient_tiles(advect, diffuse, low, high, tile, g) for g in range(GROUPS)
        ]
        from_east = eastern([values[2] for values in groups], lane)
        from_west = western([values[1] for values in groups], lane)
        for g in range(GROUPS):
            coefs[0, g, rows, :] = groups[g][0]
            coefs[1, g, rows, :] = from_east[g]
            coefs[2, g, rows, :] = from_west[g]
            coefs[3, g, rows, :] = groups[g][4]
            coefs[4, g, rows, :] = groups[g][3]
    for g in range(GROUPS):
        for which in (3, 4):
            coefs[which, g, 0:8, :] = nothing
            coefs[which, g, TALL - 8 : TALL, :] = nothing
        for k in range(COMPS):
            cell = k * GROUPS + g
            for slot in range(2):
                work[slot, cell, 0:8, :] = nothing
                work[slot, cell, TALL - 8 : TALL, :] = nothing
            work[0, cell, 8:16, :] = nothing
            work[0, cell, 32:40, :] = nothing
            inverse = jnp.broadcast_to(following[64 + k : 65 + k, lanes(g)], (8, LANES))
            for half in range(2):
                start = following[16 * k + 8 * half : 16 * k + 8 * half + 8, lanes(g)]
                end = history[STEPS - 1, cell, 8 * half : 8 * half + 8, :]
                work[0, cell, OWN + 8 * half : OWN + 8 * half + 8, :] = inverse * (end - start)
    scale = weight[0]

    def step(turn, carry):
        moment = STEPS - 1 - turn
        now = lax.rem(turn, 2)
        after = 1 - now
        pltpu.make_async_copy(
            obs_values.at[moment], observed.at[moment], arrivals.at[moment]
        ).wait()
        for entry in range(2):
            offset = pl.multiple_of(obs_rows[moment, entry] * BLOCK, BLOCK)
            for k in range(COMPS):
                for g in range(GROUPS):
                    cell = k * GROUPS + g
                    misfit = (
                        history[moment, cell, pl.ds(offset, 8), :]
                        - observed[moment, entry, k, :, lanes(g)]
                    )
                    there = pl.ds(OWN + offset, 8)
                    work[now, cell, there, :] = work[now, cell, there, :] + scale * misfit
        for tile in range(4):
            start = FIRST + 8 * tile

            def source(k, g, shift):
                return work[now, k * GROUPS + g, start + shift : start + shift + 8, :]

            def store(k, g, value):
                work[after, k * GROUPS + g, start : start + 8, :] = value

            shifts = (0, 0, 0, 1, -1)
            loads = [
                lambda g, which=which: coefs[
                    which, g, start + shifts[which] : start + shifts[which] + 8, :
                ]
                for which in range(5)
            ]
            stencil_tile(source, tile, lane, *loads, store)
        return carry

    lax.fori_loop(0, STEPS, step, 0)
    for cell in range(CELLS):
        to_low[cell] = work[0, cell, 8:16, :]
        own[cell] = work[0, cell, 16:32, :]
        to_high[cell] = work[0, cell, 32:40, :]


def gradient_kernel(inverse, own, from_low, from_high, checkpoint, prior_end, parcels):
    squares = jnp.zeros((8, LANES), jnp.float32)
    for k in range(COMPS):
        scale = inverse[0, k]
        for g in range(GROUPS):
            cell = k * GROUPS + g
            for half in range(2):
                rows = slice(8 * half, 8 * half + 8)
                other = (from_low if half == 0 else from_high)[cell]
                forcing = checkpoint[k, rows, lanes(g)] - prior_end[cell, rows, :]
                value = own[cell, rows, :] + other + scale * forcing
                place = 9 * (2 * cell + half)
                parcels[place : place + 8, :] = value
                squares = squares + value * value
    total = jnp.sum(squares, axis=0, keepdims=True)
    for parcel in range(2 * CELLS):
        parcels[9 * parcel + 8 : 9 * parcel + 9, :] = total


def smoothing_kernel(component, rates, parcels, back, total):
    windows = back.shape[0]
    which = component[0]
    running = jnp.zeros((8, LANES), jnp.float32)
    sums = jnp.zeros((1, LANES), jnp.float32)
    kept = []
    for j in range(windows):
        rate = jnp.full((8, LANES), rates[j, which], jnp.float32)
        innovation = jnp.sqrt(1.0 - rate * rate)
        running = rate * running + innovation * parcels[9 * j : 9 * j + 8, :]
        back[j] = innovation * running
        sums = sums + parcels[9 * j + 8 : 9 * j + 9, :]
    total[...] = sums
    running = back[windows - 1]
    for j in range(windows - 2, -1, -1):
        rate = jnp.full((8, LANES), rates[j + 1, which], jnp.float32)
        running = back[j] + rate * running
        back[j] = running


def final_kernel(entries, back, total, direction, rms):
    whole = jnp.broadcast_to(jnp.sum(total[...], axis=1, keepdims=True), (8, LANES))
    rms_tile = jnp.sqrt(whole / entries + 1e-06)
    share = 1.0 / rms_tile
    for k in range(COMPS):
        for g in range(GROUPS):
            for half in range(2):
                direction[k, 8 * half : 8 * half + 8, lanes(g)] = (
                    back[2 * (k * GROUPS + g) + half] * share
                )
    rms[...] = rms_tile[0:1, :]


def edge_payload(checkpoint, advect, diffuse, rows):
    return jnp.concatenate([checkpoint[:, rows], advect[:, rows], diffuse[None, rows]]).reshape(
        56, COLUMNS
    )


def on_device(checkpoint, advect, diffuse, obs_rows, obs_values, obs_weight, error_inverse, rates):
    initial, flow, spread = checkpoint[0], advect[0], diffuse[0]
    low = passed_along(edge_payload(initial, flow, spread, slice(8, 16)), SPACE, 1)
    high = passed_along(edge_payload(initial, flow, spread, slice(0, 8)), SPACE, -1)
    inverse_rows = jnp.broadcast_to(
        jnp.concatenate([error_inverse[0], error_inverse[0]])[:, None], (8, COLUMNS)
    )
    following = passed_along(
        jnp.concatenate([initial.reshape(64, COLUMNS), inverse_rows]), TM, -1
    )
    history, end_state = pl.pallas_call(
        forward_kernel,
        out_shape=(shape(STEPS, CELLS, ROWS, LANES), shape(CELLS, ROWS, LANES)),
        in_specs=[VMEM] * 5,
        out_specs=(VMEM, VMEM),
        scratch_shapes=[
            pltpu.VMEM((5, GROUPS, TALL, LANES), jnp.float32),
            pltpu.VMEM((2, CELLS, TALL, LANES), jnp.float32),
        ],
        name="forward",
    )(initial, flow, spread, low, high)
    prior_end = passed_along(end_state, TM, 1)
    own, to_low, to_high = pl.pallas_call(
        adjoint_kernel,
        out_shape=(shape(CELLS, ROWS, LANES), shape(CELLS, 8, LANES), shape(CELLS, 8, LANES)),
        in_specs=[SMEM, SMEM] + [VMEM] * 6 + [ANY],
        out_specs=(VMEM, VMEM, VMEM),
        scratch_shapes=[
            pltpu.VMEM((5, GROUPS, TALL, LANES), jnp.float32),
            pltpu.VMEM((2, CELLS, TALL, LANES), jnp.float32),
            pltpu.VMEM((STEPS, 2, COMPS, BLOCK, COLUMNS), jnp.float32),
            pltpu.SemaphoreType.DMA((STEPS,)),
        ],
        name="adjoint",
    )(obs_rows[0], obs_weight, flow, spread, low, high, history, following, obs_values[0])
    from_low = passed_along(to_high, SPACE, 1)
    from_high = passed_along(to_low, SPACE, -1)
    windows = lax.axis_size(TM)
    parcels = pl.pallas_call(
        gradient_kernel,
        out_shape=shape(9 * 2 * CELLS, LANES),
        in_specs=[SMEM] + [VMEM] * 5,
        out_specs=VMEM,
        name="gradient",
    )(error_inverse, own, from_low, from_high, initial, prior_end)
    arrived = lax.all_to_all(
        parcels.reshape(windows, 1, 9 * LANES), TM, split_axis=0, concat_axis=0, tiled=True
    )
    position = lax.axis_index(TM)
    component = (position // (windows // COMPS)).astype(jnp.int32).reshape(1)
    back, total = pl.pallas_call(
        smoothing_kernel,
        out_shape=(shape(windows, 8, LANES), shape(1, LANES)),
        in_specs=[SMEM, SMEM, VMEM],
        out_specs=(VMEM, VMEM),
        name="smoothing",
    )(component, rates, arrived.reshape(9 * windows, LANES))
    back = lax.all_to_all(back, TM, split_axis=0, concat_axis=0, tiled=True)
    total = total + swapped(total, "space_1")
    total = total + swapped(total, "space_0")
    entries = float(windows * lax.axis_size(SPACE) * initial.size)
    direction, rms = pl.pallas_call(
        lambda *refs: final_kernel(entries, *refs),
        out_shape=(shape(COMPS, ROWS, COLUMNS), shape(1, LANES)),
        in_specs=[VMEM, VMEM],
        out_specs=(VMEM, VMEM),
        name="final",
    )(back, total)
    return (direction[None], rms[0, 0])


def solution(mesh):
    torus = Mesh(
        mesh.devices.reshape(8, 2, 4, 2, 2), ("tm_0", "tm_1", "tm_2", "space_0", "space_1")
    )
    return jax.shard_map(
        on_device,
        mesh=torus,
        in_specs=(
            P(TM, None, SPACE, None),
            P(TM, None, SPACE, None),
            P(TM, SPACE, None),
            P(TM, None, SPACE),
            P(TM, None, SPACE, None, None, None),
            P(TM),
            P(TM, None),
            P(),
        ),
        out_specs=(P(TM, None, SPACE, None), P()),
        check_vma=False,
    )
```

```python
import jax
import jax.numpy as jnp
from jax import lax
from jax.experimental import pallas as pl
from jax.experimental.pallas import tpu as pltpu
from jax.sharding import Mesh
from jax.sharding import PartitionSpec as P

STEPS = 8
BLOCK = 8
COMPS = 4
ROWS = 16
LANES = 128
GROUPS = 8
COLUMNS = GROUPS * LANES
TALL = 48
FIRST = 8
OWN = 16
CELLS = COMPS * GROUPS
SPACE = ("space_0", "space_1")
TM = ("tm_0", "tm_1", "tm_2")
VMEM = pl.BlockSpec(memory_space=pltpu.VMEM)
SMEM = pl.BlockSpec(memory_space=pltpu.SMEM)
FAR = pl.BlockSpec(memory_space=pltpu.HBM)
GRANT = pltpu.CompilerParams(vmem_limit_bytes=8 * 1024 * 1024)


def shape(*dims):
    return jax.ShapeDtypeStruct(dims, jnp.float32)


def local(*dims):
    return pltpu.VMEM(dims, jnp.float32)


def near(value):
    return pltpu.with_memory_space_constraint(value, pltpu.VMEM)


def far(value):
    return pltpu.with_memory_space_constraint(value, pltpu.HBM)


def scalars(value):
    return pltpu.with_memory_space_constraint(value, pltpu.SMEM)


def lanes(group):
    return slice(group * LANES, (group + 1) * LANES)


def passed_along(value, axis, steps):
    count = lax.axis_size(axis)
    leading, last = (max(0, -steps), min(count, count - steps))
    return lax.ppermute(value, axis, [(source, source + steps) for source in range(leading, last)])


def swapped(value, axis):
    return lax.ppermute(value, axis, [(0, 1), (1, 0)])


def crossed(value):
    return lax.ppermute(value, SPACE, [(1, 2), (2, 1)])


def side_rows():
    odd = lax.axis_index("space_1")
    return pl.multiple_of(32 - 24 * odd, 8), pl.multiple_of(8 + 24 * odd, 8)


def eastern(tiles, lane):
    turned = [pltpu.roll(tile, LANES - 1, 1) for tile in tiles]
    return [
        jnp.where(lane == LANES - 1, turned[(g + 1) % GROUPS], turned[g]) for g in range(GROUPS)
    ]


def western(tiles, lane):
    turned = [pltpu.roll(tile, 1, 1) for tile in tiles]
    return [jnp.where(lane == 0, turned[g - 1], turned[g]) for g in range(GROUPS)]


def coefficient_tiles(advect, diffuse, pair, other, tile, group):
    if tile < 2:
        rows = slice(tile * 8, tile * 8 + 8)
        east_flow = advect[0, rows, lanes(group)]
        north_flow = advect[1, rows, lanes(group)]
        spread = diffuse[rows, lanes(group)]
    else:
        side = pair if tile == 2 else other
        east_flow = side[32:40, lanes(group)]
        north_flow = side[40:48, lanes(group)]
        spread = side[48:56, lanes(group)]
    return (
        1.0 - 4.0 * spread,
        spread - 0.5 * east_flow,
        spread + 0.5 * east_flow,
        spread - 0.5 * north_flow,
        spread + 0.5 * north_flow,
    )


def lane_index():
    return lax.broadcasted_iota(jnp.int32, (8, LANES), 1)


def stencil_tile(source, lane, centre, east, west, north, south, store):
    fields = [[source(k, g, 0) for g in range(GROUPS)] for k in range(COMPS)]
    to_east = [eastern(row, lane) for row in fields]
    to_west = [western(row, lane) for row in fields]
    for g in range(GROUPS):
        c, e, w, n, s = centre(g), east(g), west(g), north(g), south(g)
        for k in range(COMPS):
            store(
                k,
                g,
                c * fields[k][g]
                + e * to_east[k][g]
                + w * to_west[k][g]
                + n * source(k, g, 1)
                + s * source(k, g, -1),
            )


def edges_kernel(
    inverse, checkpoint, advect, diffuse,
    to_pair, to_other, to_prior, own_checkpoint, own_advect, own_diffuse, settings,
    inverse_row, arrivals,
):
    copies = []

    def fetch(source, target):
        copies.append(pltpu.make_async_copy(source, target, arrivals.at[len(copies)]))
        copies[-1].start()

    fetch(inverse, inverse_row)
    odd = lax.axis_index("space_1")
    for half, side in ((odd, to_other), (1 - odd, to_pair)):
        rows = pl.ds(pl.multiple_of(8 * half, 8), 8)
        for k in range(COMPS):
            fetch(checkpoint.at[k, rows], side.at[pl.ds(8 * k, 8)])
        for axis in range(2):
            fetch(advect.at[axis, rows], side.at[pl.ds(32 + 8 * axis, 8)])
        fetch(diffuse.at[rows], side.at[pl.ds(48, 8)])
    fetch(checkpoint, to_prior.at[pl.ds(0, COMPS)])
    fetch(checkpoint, own_checkpoint)
    fetch(advect, own_advect)
    fetch(diffuse, own_diffuse)
    copies[0].wait()
    for k in range(COMPS):
        spread = jnp.broadcast_to(inverse_row[0:1, k : k + 1], (8, LANES))
        to_prior[COMPS, 0:8, lanes(k)] = spread
        settings[k] = spread
    for copy in copies[1:]:
        copy.wait()


def forward_kernel(
    checkpoint, advect, diffuse, pair, other, obs_values,
    history, last, observed, coefs, work, arrival,
):
    fetch = pltpu.make_async_copy(obs_values, observed, arrival)
    fetch.start()
    lane = lane_index()
    nothing = jnp.zeros((8, LANES), jnp.float32)
    starts = (OWN, OWN + 8) + side_rows()
    for g in range(GROUPS):
        for tile in range(4):
            rows = pl.ds(starts[tile], 8)
            values = coefficient_tiles(advect, diffuse, pair, other, tile, g)
            for which in range(5):
                coefs[which, g, rows, :] = values[which]
            for k in range(COMPS):
                if tile < 2:
                    value = checkpoint[k, tile * 8 : tile * 8 + 8, lanes(g)]
                else:
                    value = (pair if tile == 2 else other)[8 * k : 8 * k + 8, lanes(g)]
                work[0, k * GROUPS + g, rows, :] = value
        for k in range(COMPS):
            for slot in range(2):
                work[slot, k * GROUPS + g, 0:8, :] = nothing
                work[slot, k * GROUPS + g, TALL - 8 : TALL, :] = nothing

    def step(moment, carry):
        now = lax.rem(moment, 2)
        after = 1 - now
        for tile in range(4):
            start = FIRST + 8 * tile

            def source(k, g, shift):
                return work[now, k * GROUPS + g, start + shift : start + shift + 8, :]

            def store(k, g, value):
                work[after, k * GROUPS + g, start : start + 8, :] = value
                if tile in (1, 2):
                    history[moment, k * GROUPS + g, (tile - 1) * 8 : tile * 8, :] = value

            loads = [
                lambda g, which=which: coefs[which, g, start : start + 8, :] for which in range(5)
            ]
            stencil_tile(source, lane, *loads, store)
        return carry

    lax.fori_loop(0, STEPS, step, 0)
    for cell in range(CELLS):
        last[cell] = history[STEPS - 1, cell]
    fetch.wait()


def adjoint_kernel(
    obs_rows, weight, advect, diffuse, pair, other, history, following, obs_values,
    own, to_pair, to_other, coefs, work,
):
    lane = lane_index()
    nothing = jnp.zeros((8, LANES), jnp.float32)
    starts = (OWN, OWN + 8) + side_rows()
    for tile in range(4):
        rows = pl.ds(starts[tile], 8)
        groups = [
            coefficient_tiles(advect, diffuse, pair, other, tile, g) for g in range(GROUPS)
        ]
        from_east = eastern([values[2] for values in groups], lane)
        from_west = western([values[1] for values in groups], lane)
        for g in range(GROUPS):
            coefs[0, g, rows, :] = groups[g][0]
            coefs[1, g, rows, :] = from_east[g]
            coefs[2, g, rows, :] = from_west[g]
            coefs[3, g, rows, :] = groups[g][4]
            coefs[4, g, rows, :] = groups[g][3]
    inverses = [following[COMPS, 0:8, lanes(k)] for k in range(COMPS)]
    for g in range(GROUPS):
        for which in (3, 4):
            coefs[which, g, 0:8, :] = nothing
            coefs[which, g, TALL - 8 : TALL, :] = nothing
        for k in range(COMPS):
            cell = k * GROUPS + g
            for slot in range(2):
                work[slot, cell, 0:8, :] = nothing
                work[slot, cell, TALL - 8 : TALL, :] = nothing
            work[0, cell, 8:16, :] = nothing
            work[0, cell, 32:40, :] = nothing
            for half in range(2):
                start = following[k, 8 * half : 8 * half + 8, lanes(g)]
                end = history[STEPS - 1, cell, 8 * half : 8 * half + 8, :]
                work[0, cell, OWN + 8 * half : OWN + 8 * half + 8, :] = inverses[k] * (end - start)
    scale = jnp.broadcast_to(weight[...], (8, LANES))

    def step(turn, carry):
        moment = STEPS - 1 - turn
        now = lax.rem(turn, 2)
        after = 1 - now
        for entry in range(2):
            offset = pl.multiple_of(obs_rows[entry, moment] * BLOCK, BLOCK)
            for k in range(COMPS):
                for g in range(GROUPS):
                    cell = k * GROUPS + g
                    misfit = (
                        history[moment, cell, pl.ds(offset, 8), :]
                        - obs_values[moment, entry, k, :, lanes(g)]
                    )
                    there = pl.ds(OWN + offset, 8)
                    work[now, cell, there, :] = work[now, cell, there, :] + scale * misfit
        for tile in range(4):
            start = FIRST + 8 * tile

            def source(k, g, shift):
                return work[now, k * GROUPS + g, start + shift : start + shift + 8, :]

            def store(k, g, value):
                work[after, k * GROUPS + g, start : start + 8, :] = value

            shifts = (0, 0, 0, 1, -1)
            loads = [
                lambda g, which=which: coefs[
                    which, g, start + shifts[which] : start + shifts[which] + 8, :
                ]
                for which in range(5)
            ]
            stencil_tile(source, lane, *loads, store)
        return carry

    lax.fori_loop(0, STEPS, step, 0)
    for cell in range(CELLS):
        to_pair[cell] = work[0, cell, pl.ds(starts[2], 8), :]
        to_other[cell] = work[0, cell, pl.ds(starts[3], 8), :]
        own[cell] = work[0, cell, 16:32, :]


def gradient_kernel(settings, own, from_pair, from_other, checkpoint, prior_end, parcels):
    even = jnp.full((8, LANES), lax.axis_index("space_1")) == 0
    squares = jnp.zeros((8, LANES), jnp.float32)
    for k in range(COMPS):
        scale = settings[k]
        for g in range(GROUPS):
            cell = k * GROUPS + g
            pair, other = from_pair[cell], from_other[cell]
            added = (jnp.where(even, other, pair), jnp.where(even, pair, other))
            for half in range(2):
                rows = slice(8 * half, 8 * half + 8)
                forcing = checkpoint[k, rows, lanes(g)] - prior_end[cell, rows, :]
                value = own[cell, rows, :] + added[half] + scale * forcing
                place = 9 * (2 * cell + half)
                parcels[place : place + 8, :] = value
                squares = squares + value * value
    total = jnp.sum(squares, axis=0, keepdims=True)
    for parcel in range(2 * CELLS):
        parcels[9 * parcel + 8 : 9 * parcel + 9, :] = total


def smoothing_kernel(rates, parcels, back, total):
    windows = back.shape[0]
    which = lax.axis_index(TM) // (windows // COMPS)
    running = jnp.zeros((8, LANES), jnp.float32)
    sums = jnp.zeros((1, LANES), jnp.float32)
    for j in range(windows):
        rate = jnp.full((8, LANES), rates[which, j], jnp.float32)
        innovation = jnp.sqrt(1.0 - rate * rate)
        running = rate * running + innovation * parcels[9 * j : 9 * j + 8, :]
        back[j] = innovation * running
        sums = sums + parcels[9 * j + 8 : 9 * j + 9, :]
    total[...] = sums
    running = back[windows - 1]
    for j in range(windows - 2, -1, -1):
        rate = jnp.full((8, LANES), rates[which, j + 1], jnp.float32)
        running = back[j] + rate * running
        back[j] = running


def final_kernel(entries, back, total, direction, rms):
    whole = jnp.broadcast_to(jnp.sum(total[...], axis=1, keepdims=True), (8, LANES))
    rms_tile = jnp.sqrt(whole / entries + 1e-06)
    share = 1.0 / rms_tile
    for k in range(COMPS):
        for g in range(GROUPS):
            for half in range(2):
                direction[k, 8 * half : 8 * half + 8, lanes(g)] = (
                    back[2 * (k * GROUPS + g) + half] * share
                )
    rms[...] = rms_tile[0:1, :]


def on_device(checkpoint, advect, diffuse, obs_rows, obs_values, obs_weight, error_inverse, rates):
    edge_pair, edge_other, start, initial, flow, spread, settings = pl.pallas_call(
        edges_kernel,
        out_shape=(
            local(56, COLUMNS), local(56, COLUMNS), local(COMPS + 1, ROWS, COLUMNS),
            local(COMPS, ROWS, COLUMNS), local(2, ROWS, COLUMNS), local(ROWS, COLUMNS),
            local(COMPS, 8, LANES),
        ),
        in_specs=[FAR] * 4,
        out_specs=(VMEM,) * 7,
        scratch_shapes=[
            pltpu.VMEM((1, COMPS), jnp.float32),
            pltpu.SemaphoreType.DMA((19,)),
        ],
        name="edges",
        compiler_params=GRANT,
    )(
        far(error_inverse), far(checkpoint[0]), far(advect[0]), far(diffuse[0])
    )
    initial, flow, spread, settings = near(initial), near(flow), near(spread), near(settings)
    other = near(crossed(edge_other))
    pair = near(swapped(edge_pair, "space_1"))
    following = near(passed_along(start, TM, -1))
    weight = near(jnp.broadcast_to(obs_weight[None], (1, LANES)))
    history, end_state, observed = pl.pallas_call(
        forward_kernel,
        out_shape=(
            local(STEPS, CELLS, ROWS, LANES), local(CELLS, ROWS, LANES),
            local(STEPS, 2, COMPS, BLOCK, COLUMNS),
        ),
        in_specs=[VMEM] * 5 + [FAR],
        out_specs=(VMEM,) * 3,
        scratch_shapes=[
            pltpu.VMEM((5, GROUPS, TALL, LANES), jnp.float32),
            pltpu.VMEM((2, CELLS, TALL, LANES), jnp.float32),
            pltpu.SemaphoreType.DMA(()),
        ],
        name="forward",
        compiler_params=GRANT,
    )(initial, flow, spread, pair, other, far(obs_values[0]))
    prior_end = near(passed_along(end_state, TM, 1))
    own, to_pair, to_other = pl.pallas_call(
        adjoint_kernel,
        out_shape=(local(CELLS, ROWS, LANES), local(CELLS, 8, LANES), local(CELLS, 8, LANES)),
        in_specs=[SMEM] + [VMEM] * 8,
        out_specs=(VMEM, VMEM, VMEM),
        scratch_shapes=[
            pltpu.VMEM((5, GROUPS, TALL, LANES), jnp.float32),
            pltpu.VMEM((2, CELLS, TALL, LANES), jnp.float32),
        ],
        name="adjoint",
        compiler_params=GRANT,
    )(
        scalars(obs_rows[0].T), weight, flow, spread, pair, other,
        near(history), following, near(observed),
    )
    from_other = near(crossed(to_other))
    from_pair = near(swapped(to_pair, "space_1"))
    windows = lax.axis_size(TM)
    parcels = pl.pallas_call(
        gradient_kernel,
        out_shape=local(9 * 2 * CELLS, LANES),
        in_specs=[VMEM] * 6,
        out_specs=VMEM,
        name="gradient",
        compiler_params=GRANT,
    )(settings, near(own), from_pair, from_other, initial, prior_end)
    arrived = lax.all_to_all(
        parcels.reshape(windows, 1, 9 * LANES), TM, split_axis=0, concat_axis=0, tiled=True
    )
    back, total = pl.pallas_call(
        smoothing_kernel,
        out_shape=(local(windows, 8, LANES), local(1, LANES)),
        in_specs=[SMEM, VMEM],
        out_specs=(VMEM, VMEM),
        name="smoothing",
        compiler_params=GRANT,
    )(scalars(rates.T), near(arrived.reshape(9 * windows, LANES)))
    back = near(lax.all_to_all(back, TM, split_axis=0, concat_axis=0, tiled=True))
    total = total + swapped(total, "space_1")
    total = near(total + swapped(total, "space_0"))
    entries = float(windows * lax.axis_size(SPACE) * checkpoint.size)
    direction, rms = pl.pallas_call(
        lambda *refs: final_kernel(entries, *refs),
        out_shape=(shape(COMPS, ROWS, COLUMNS), shape(1, LANES)),
        in_specs=[VMEM, VMEM],
        out_specs=(VMEM, VMEM),
        name="final",
        compiler_params=GRANT,
    )(back, total)
    return (direction[None], rms[0, 0])


def solution(mesh):
    torus = Mesh(
        mesh.devices.reshape(8, 2, 4, 2, 2), ("tm_0", "tm_1", "tm_2", "space_0", "space_1")
    )

    return jax.shard_map(
        on_device,
        mesh=torus,
        in_specs=(
            P(TM, None, SPACE, None),
            P(TM, None, SPACE, None),
            P(TM, SPACE, None),
            P(TM, None, SPACE),
            P(TM, None, SPACE, None, None, None),
            P(TM),
            P(TM, None),
            P(),
        ),
        out_specs=(P(TM, None, SPACE, None), P()),
        check_vma=False,
    )
```

```python
import jax
import jax.numpy as jnp
from jax import lax
from jax.experimental import pallas as pl
from jax.experimental.pallas import tpu as pltpu
from jax.sharding import Mesh
from jax.sharding import PartitionSpec as P

STEPS = 8
BLOCK = 8
COMPS = 4
ROWS = 16
LANES = 128
GROUPS = 8
COLUMNS = GROUPS * LANES
TALL = 48
FIRST = 8
OWN = 16
CELLS = COMPS * GROUPS
TOGETHER = 4
SPACE = ("space_0", "space_1")
TM = ("tm_0", "tm_1", "tm_2")
VMEM = pl.BlockSpec(memory_space=pltpu.VMEM)
SMEM = pl.BlockSpec(memory_space=pltpu.SMEM)
FAR = pl.BlockSpec(memory_space=pltpu.HBM)
GRANT = pltpu.CompilerParams(vmem_limit_bytes=8 * 1024 * 1024)


def shape(*dims):
    return jax.ShapeDtypeStruct(dims, jnp.float32)


def local(*dims):
    return pltpu.VMEM(dims, jnp.float32)


def near(value):
    return pltpu.with_memory_space_constraint(value, pltpu.VMEM)


def far(value):
    return pltpu.with_memory_space_constraint(value, pltpu.HBM)


def scalars(value):
    return pltpu.with_memory_space_constraint(value, pltpu.SMEM)


def lanes(group):
    return slice(group * LANES, (group + 1) * LANES)


def passed_along(value, axis, steps):
    count = lax.axis_size(axis)
    leading, last = (max(0, -steps), min(count, count - steps))
    return lax.ppermute(value, axis, [(source, source + steps) for source in range(leading, last)])


def swapped(value, axis):
    return lax.ppermute(value, axis, [(0, 1), (1, 0)])


def crossed(value):
    return lax.ppermute(value, SPACE, [(1, 2), (2, 1)])


def side_rows():
    odd = lax.axis_index("space_1")
    return pl.multiple_of(32 - 24 * odd, 8), pl.multiple_of(8 + 24 * odd, 8)


def eastern(tiles, lane):
    turned = [pltpu.roll(tile, LANES - 1, 1) for tile in tiles]
    return [
        jnp.where(lane == LANES - 1, turned[(g + 1) % GROUPS], turned[g]) for g in range(GROUPS)
    ]


def western(tiles, lane):
    turned = [pltpu.roll(tile, 1, 1) for tile in tiles]
    return [jnp.where(lane == 0, turned[g - 1], turned[g]) for g in range(GROUPS)]


def coefficient_tiles(advect, diffuse, pair, other, tile, group):
    if tile < 2:
        rows = slice(tile * 8, tile * 8 + 8)
        east_flow = advect[0, rows, lanes(group)]
        north_flow = advect[1, rows, lanes(group)]
        spread = diffuse[rows, lanes(group)]
    else:
        side = pair if tile == 2 else other
        east_flow = side[32:40, lanes(group)]
        north_flow = side[40:48, lanes(group)]
        spread = side[48:56, lanes(group)]
    return (
        1.0 - 4.0 * spread,
        spread - 0.5 * east_flow,
        spread + 0.5 * east_flow,
        spread - 0.5 * north_flow,
        spread + 0.5 * north_flow,
    )


def lane_index():
    return lax.broadcasted_iota(jnp.int32, (8, LANES), 1)


def stencil_step(source, target, coefs, shifts, first, tiles, lane):
    def components(turn, carry):
        for k in range(TOGETHER):
            cell = (turn * TOGETHER + k) * GROUPS
            for tile in range(tiles):
                start = FIRST + first + 8 * tile
                field = [source[cell + g, start : start + 8, :] for g in range(GROUPS)]
                to_east = eastern(field, lane)
                to_west = western(field, lane)
                for g in range(GROUPS):
                    c, e, w, n, s = (
                        coefs[which, g, start + shifts[which] : start + shifts[which] + 8, :]
                        for which in range(5)
                    )
                    target[cell + g, start : start + 8, :] = (
                        c * field[g]
                        + e * to_east[g]
                        + w * to_west[g]
                        + n * source[cell + g, start + 1 : start + 9, :]
                        + s * source[cell + g, start - 1 : start + 7, :]
                    )
        return carry

    lax.fori_loop(0, COMPS // TOGETHER, components, 0)


def edges_kernel(
    inverse, checkpoint, advect, diffuse,
    to_pair, to_other, to_prior, own_checkpoint, own_advect, own_diffuse, settings,
    inverse_row, arrivals,
):
    copies = []

    def fetch(source, target):
        copies.append(pltpu.make_async_copy(source, target, arrivals.at[len(copies)]))
        copies[-1].start()

    fetch(inverse, inverse_row)
    odd = lax.axis_index("space_1")
    for half, side in ((odd, to_other), (1 - odd, to_pair)):
        rows = pl.ds(pl.multiple_of(8 * half, 8), 8)
        for k in range(COMPS):
            fetch(checkpoint.at[k, rows], side.at[pl.ds(8 * k, 8)])
        for axis in range(2):
            fetch(advect.at[axis, rows], side.at[pl.ds(32 + 8 * axis, 8)])
        fetch(diffuse.at[rows], side.at[pl.ds(48, 8)])
    fetch(checkpoint, to_prior.at[pl.ds(0, COMPS)])
    fetch(checkpoint, own_checkpoint)
    fetch(advect, own_advect)
    fetch(diffuse, own_diffuse)
    copies[0].wait()
    for k in range(COMPS):
        spread = jnp.broadcast_to(inverse_row[0:1, k : k + 1], (8, LANES))
        to_prior[COMPS, 0:8, lanes(k)] = spread
        settings[k] = spread
    for copy in copies[1:]:
        copy.wait()


def forward_kernel(
    checkpoint, advect, diffuse, pair, other, obs_values,
    history, last, observed, coefs, initial, arrival,
):
    fetch = pltpu.make_async_copy(obs_values, observed, arrival)
    fetch.start()
    lane = lane_index()
    nothing = jnp.zeros((8, LANES), jnp.float32)
    starts = (OWN, OWN + 8) + side_rows()
    for g in range(GROUPS):
        for tile in range(4):
            rows = pl.ds(starts[tile], 8)
            values = coefficient_tiles(advect, diffuse, pair, other, tile, g)
            for which in range(5):
                coefs[which, g, rows, :] = values[which]
            for k in range(COMPS):
                if tile < 2:
                    value = checkpoint[k, tile * 8 : tile * 8 + 8, lanes(g)]
                else:
                    value = (pair if tile == 2 else other)[8 * k : 8 * k + 8, lanes(g)]
                initial[k * GROUPS + g, rows, :] = value
        for k in range(COMPS):
            initial[k * GROUPS + g, 0:8, :] = nothing
            initial[k * GROUPS + g, TALL - 8 : TALL, :] = nothing

    for moment in range(STEPS):
        first, tiles = ((0, 4), (4, 3), (8, 2))[(moment >= 3) + (moment >= 7)]
        if tiles == 3:
            first = moment + 1
        source = history.at[moment - 1] if moment else initial
        stencil_step(source, history.at[moment], coefs, (0,) * 5, first, tiles, lane)
    for cell in range(CELLS):
        last[cell] = history[STEPS - 1, cell, OWN : OWN + 16, :]
    fetch.wait()


def adjoint_kernel(
    obs_rows, weight, advect, diffuse, pair, other, history, following, obs_values,
    own, to_pair, to_other, coefs, work,
):
    lane = lane_index()
    nothing = jnp.zeros((8, LANES), jnp.float32)
    starts = (OWN, OWN + 8) + side_rows()
    for tile in range(4):
        rows = pl.ds(starts[tile], 8)
        groups = [
            coefficient_tiles(advect, diffuse, pair, other, tile, g) for g in range(GROUPS)
        ]
        from_east = eastern([values[2] for values in groups], lane)
        from_west = western([values[1] for values in groups], lane)
        for g in range(GROUPS):
            coefs[0, g, rows, :] = groups[g][0]
            coefs[1, g, rows, :] = from_east[g]
            coefs[2, g, rows, :] = from_west[g]
            coefs[3, g, rows, :] = groups[g][4]
            coefs[4, g, rows, :] = groups[g][3]
    inverses = [following[COMPS, 0:8, lanes(k)] for k in range(COMPS)]
    for g in range(GROUPS):
        for which in (3, 4):
            coefs[which, g, 0:8, :] = nothing
            coefs[which, g, TALL - 8 : TALL, :] = nothing
        for k in range(COMPS):
            cell = k * GROUPS + g
            for slot in range(2):
                for rows in (slice(0, 8), slice(8, 16), slice(32, 40), slice(TALL - 8, TALL)):
                    work[slot, cell, rows, :] = nothing
            for half in range(2):
                start = following[k, 8 * half : 8 * half + 8, lanes(g)]
                end = history[STEPS - 1, cell, OWN + 8 * half : OWN + 8 * half + 8, :]
                work[0, cell, OWN + 8 * half : OWN + 8 * half + 8, :] = inverses[k] * (end - start)
    scale = jnp.broadcast_to(weight[...], (8, LANES))

    for turn in range(STEPS):
        moment = STEPS - 1 - turn
        now = turn % 2
        for entry in range(2):
            offset = pl.multiple_of(obs_rows[entry, moment] * BLOCK, BLOCK)
            there = pl.ds(OWN + offset, 8)
            for k in range(COMPS):
                for g in range(GROUPS):
                    cell = k * GROUPS + g
                    misfit = history[moment, cell, there, :] - obs_values[
                        moment, entry, k, :, lanes(g)
                    ]
                    work[now, cell, there, :] = work[now, cell, there, :] + scale * misfit
        first, tiles = (7 - turn, 3) if turn < 4 else (0, 4)
        stencil_step(
            work.at[now], work.at[1 - now], coefs, (0, 0, 0, 1, -1), first, tiles, lane
        )
    for cell in range(CELLS):
        to_pair[cell] = work[0, cell, pl.ds(starts[2], 8), :]
        to_other[cell] = work[0, cell, pl.ds(starts[3], 8), :]
        own[cell] = work[0, cell, 16:32, :]


def gradient_kernel(settings, own, from_pair, from_other, checkpoint, prior_end, parcels):
    even = jnp.full((8, LANES), lax.axis_index("space_1")) == 0
    squares = jnp.zeros((8, LANES), jnp.float32)
    for k in range(COMPS):
        scale = settings[k]
        for g in range(GROUPS):
            cell = k * GROUPS + g
            pair, other = from_pair[cell], from_other[cell]
            added = (jnp.where(even, other, pair), jnp.where(even, pair, other))
            for half in range(2):
                rows = slice(8 * half, 8 * half + 8)
                forcing = checkpoint[k, rows, lanes(g)] - prior_end[cell, rows, :]
                value = own[cell, rows, :] + added[half] + scale * forcing
                place = 9 * (2 * cell + half)
                parcels[place : place + 8, :] = value
                squares = squares + value * value
    total = jnp.sum(squares, axis=0, keepdims=True)
    for parcel in range(2 * CELLS):
        parcels[9 * parcel + 8 : 9 * parcel + 9, :] = total


def smoothing_kernel(rates, parcels, back, total):
    windows = back.shape[0]
    which = lax.axis_index(TM) // (windows // COMPS)
    running = jnp.zeros((8, LANES), jnp.float32)
    sums = jnp.zeros((1, LANES), jnp.float32)
    for j in range(windows):
        rate = jnp.full((8, LANES), rates[which, j], jnp.float32)
        innovation = jnp.sqrt(1.0 - rate * rate)
        running = rate * running + innovation * parcels[9 * j : 9 * j + 8, :]
        back[j] = innovation * running
        sums = sums + parcels[9 * j + 8 : 9 * j + 9, :]
    total[...] = sums
    running = back[windows - 1]
    for j in range(windows - 2, -1, -1):
        rate = jnp.full((8, LANES), rates[which, j + 1], jnp.float32)
        running = back[j] + rate * running
        back[j] = running


def final_kernel(entries, back, total, direction, rms):
    whole = jnp.broadcast_to(jnp.sum(total[...], axis=1, keepdims=True), (8, LANES))
    rms_tile = jnp.sqrt(whole / entries + 1e-06)
    share = 1.0 / rms_tile
    for k in range(COMPS):
        for g in range(GROUPS):
            for half in range(2):
                direction[k, 8 * half : 8 * half + 8, lanes(g)] = (
                    back[2 * (k * GROUPS + g) + half] * share
                )
    rms[...] = rms_tile[0:1, :]


def on_device(checkpoint, advect, diffuse, obs_rows, obs_values, obs_weight, error_inverse, rates):
    edge_pair, edge_other, start, initial, flow, spread, settings = pl.pallas_call(
        edges_kernel,
        out_shape=(
            local(56, COLUMNS), local(56, COLUMNS), local(COMPS + 1, ROWS, COLUMNS),
            local(COMPS, ROWS, COLUMNS), local(2, ROWS, COLUMNS), local(ROWS, COLUMNS),
            local(COMPS, 8, LANES),
        ),
        in_specs=[FAR] * 4,
        out_specs=(VMEM,) * 7,
        scratch_shapes=[
            pltpu.VMEM((1, COMPS), jnp.float32),
            pltpu.SemaphoreType.DMA((19,)),
        ],
        name="edges",
        compiler_params=GRANT,
    )(
        far(error_inverse), far(checkpoint[0]), far(advect[0]), far(diffuse[0])
    )
    initial, flow, spread, settings = near(initial), near(flow), near(spread), near(settings)
    other = near(crossed(edge_other))
    pair = near(swapped(edge_pair, "space_1"))
    following = near(passed_along(start, TM, -1))
    weight = near(jnp.broadcast_to(obs_weight[None], (1, LANES)))
    history, end_state, observed = pl.pallas_call(
        forward_kernel,
        out_shape=(
            local(STEPS, CELLS, TALL, LANES), local(CELLS, ROWS, LANES),
            local(STEPS, 2, COMPS, BLOCK, COLUMNS),
        ),
        in_specs=[VMEM] * 5 + [FAR],
        out_specs=(VMEM,) * 3,
        scratch_shapes=[
            pltpu.VMEM((5, GROUPS, TALL, LANES), jnp.float32),
            pltpu.VMEM((CELLS, TALL, LANES), jnp.float32),
            pltpu.SemaphoreType.DMA(()),
        ],
        name="forward",
        compiler_params=GRANT,
    )(initial, flow, spread, pair, other, far(obs_values[0]))
    prior_end = near(passed_along(end_state, TM, 1))
    own, to_pair, to_other = pl.pallas_call(
        adjoint_kernel,
        out_shape=(local(CELLS, ROWS, LANES), local(CELLS, 8, LANES), local(CELLS, 8, LANES)),
        in_specs=[SMEM] + [VMEM] * 8,
        out_specs=(VMEM, VMEM, VMEM),
        scratch_shapes=[
            pltpu.VMEM((5, GROUPS, TALL, LANES), jnp.float32),
            pltpu.VMEM((2, CELLS, TALL, LANES), jnp.float32),
        ],
        name="adjoint",
        compiler_params=GRANT,
    )(
        scalars(obs_rows[0].T), weight, flow, spread, pair, other,
        near(history), following, near(observed),
    )
    from_other = near(crossed(to_other))
    from_pair = near(swapped(to_pair, "space_1"))
    windows = lax.axis_size(TM)
    parcels = pl.pallas_call(
        gradient_kernel,
        out_shape=local(9 * 2 * CELLS, LANES),
        in_specs=[VMEM] * 6,
        out_specs=VMEM,
        name="gradient",
        compiler_params=GRANT,
    )(settings, near(own), from_pair, from_other, initial, prior_end)
    arrived = lax.all_to_all(
        parcels.reshape(windows, 1, 9 * LANES), TM, split_axis=0, concat_axis=0, tiled=True
    )
    back, total = pl.pallas_call(
        smoothing_kernel,
        out_shape=(local(windows, 8, LANES), local(1, LANES)),
        in_specs=[SMEM, VMEM],
        out_specs=(VMEM, VMEM),
        name="smoothing",
        compiler_params=GRANT,
    )(scalars(rates.T), near(arrived.reshape(9 * windows, LANES)))
    back = near(lax.all_to_all(back, TM, split_axis=0, concat_axis=0, tiled=True))
    total = total + swapped(total, "space_1")
    total = near(total + swapped(total, "space_0"))
    entries = float(windows * lax.axis_size(SPACE) * checkpoint.size)
    direction, rms = pl.pallas_call(
        lambda *refs: final_kernel(entries, *refs),
        out_shape=(shape(COMPS, ROWS, COLUMNS), shape(1, LANES)),
        in_specs=[VMEM, VMEM],
        out_specs=(VMEM, VMEM),
        name="final",
        compiler_params=GRANT,
    )(back, total)
    return (direction[None], rms[0, 0])


def solution(mesh):
    torus = Mesh(
        mesh.devices.reshape(8, 2, 4, 2, 2), ("tm_0", "tm_1", "tm_2", "space_0", "space_1")
    )

    return jax.shard_map(
        on_device,
        mesh=torus,
        in_specs=(
            P(TM, None, SPACE, None),
            P(TM, None, SPACE, None),
            P(TM, SPACE, None),
            P(TM, None, SPACE),
            P(TM, None, SPACE, None, None, None),
            P(TM),
            P(TM, None),
            P(),
        ),
        out_specs=(P(TM, None, SPACE, None), P()),
        check_vma=False,
    )
```

```python
import jax
import jax.numpy as jnp
from jax import lax
from jax.experimental import pallas as pl
from jax.experimental.pallas import tpu as pltpu
from jax.sharding import Mesh
from jax.sharding import PartitionSpec as P

STEPS = 8
BLOCK = 8
COMPS = 4
ROWS = 16
LANES = 128
GROUPS = 8
COLUMNS = GROUPS * LANES
TALL = 48
FIRST = 8
OWN = 16
CELLS = COMPS * GROUPS
TOGETHER = 4
SPACE = ("space_0", "space_1")
TM = ("tm_0", "tm_1", "tm_2")
VMEM = pl.BlockSpec(memory_space=pltpu.VMEM)
SMEM = pl.BlockSpec(memory_space=pltpu.SMEM)
FAR = pl.BlockSpec(memory_space=pltpu.HBM)
GRANT = pltpu.CompilerParams(vmem_limit_bytes=8 * 1024 * 1024)


def shape(*dims):
    return jax.ShapeDtypeStruct(dims, jnp.float32)


def local(*dims):
    return pltpu.VMEM(dims, jnp.float32)


def near(value):
    return pltpu.with_memory_space_constraint(value, pltpu.VMEM)


def far(value):
    return pltpu.with_memory_space_constraint(value, pltpu.HBM)


def scalars(value):
    return pltpu.with_memory_space_constraint(value, pltpu.SMEM)


def lanes(group):
    return slice(group * LANES, (group + 1) * LANES)


def passed_along(value, axis, steps):
    count = lax.axis_size(axis)
    leading, last = (max(0, -steps), min(count, count - steps))
    return lax.ppermute(value, axis, [(source, source + steps) for source in range(leading, last)])


def swapped(value, axis):
    return lax.ppermute(value, axis, [(0, 1), (1, 0)])


def crossed(value):
    return lax.ppermute(value, SPACE, [(1, 2), (2, 1)])


def side_rows():
    odd = lax.axis_index("space_1")
    return pl.multiple_of(32 - 24 * odd, 8), pl.multiple_of(8 + 24 * odd, 8)


def eastern(tiles, lane):
    turned = [pltpu.roll(tile, LANES - 1, 1) for tile in tiles]
    return [
        jnp.where(lane == LANES - 1, turned[(g + 1) % GROUPS], turned[g]) for g in range(GROUPS)
    ]


def western(tiles, lane):
    turned = [pltpu.roll(tile, 1, 1) for tile in tiles]
    return [jnp.where(lane == 0, turned[g - 1], turned[g]) for g in range(GROUPS)]


def coefficient_tiles(advect, diffuse, pair, other, tile, group):
    if tile < 2:
        rows = slice(tile * 8, tile * 8 + 8)
        east_flow = advect[0, rows, lanes(group)]
        north_flow = advect[1, rows, lanes(group)]
        spread = diffuse[rows, lanes(group)]
    else:
        side = pair if tile == 2 else other
        east_flow = side[32:40, lanes(group)]
        north_flow = side[40:48, lanes(group)]
        spread = side[48:56, lanes(group)]
    return (
        1.0 - 4.0 * spread,
        spread - 0.5 * east_flow,
        spread + 0.5 * east_flow,
        spread - 0.5 * north_flow,
        spread + 0.5 * north_flow,
    )


def lane_index():
    return lax.broadcasted_iota(jnp.int32, (8, LANES), 1)


def stencil_step(source, target, coefs, shifts, first, tiles, lane):
    def components(turn, carry):
        for k in range(TOGETHER):
            cell = (turn * TOGETHER + k) * GROUPS
            for tile in range(tiles):
                start = FIRST + first + 8 * tile
                field = [source[cell + g, start : start + 8, :] for g in range(GROUPS)]
                to_east = eastern(field, lane)
                to_west = western(field, lane)
                for g in range(GROUPS):
                    c, e, w, n, s = (
                        coefs[which, g, start + shifts[which] : start + shifts[which] + 8, :]
                        for which in range(5)
                    )
                    target[cell + g, start : start + 8, :] = (
                        c * field[g]
                        + e * to_east[g]
                        + w * to_west[g]
                        + n * source[cell + g, start + 1 : start + 9, :]
                        + s * source[cell + g, start - 1 : start + 7, :]
                    )
        return carry

    lax.fori_loop(0, COMPS // TOGETHER, components, 0)


def edges_kernel(
    inverse, checkpoint, advect, diffuse,
    to_pair, to_other, to_prior, own_checkpoint, own_advect, own_diffuse, settings,
    inverse_row, arrivals,
):
    copies = []

    def fetch(source, target):
        copies.append(pltpu.make_async_copy(source, target, arrivals.at[len(copies)]))
        copies[-1].start()

    fetch(inverse, inverse_row)
    odd = lax.axis_index("space_1")
    for half, side in ((odd, to_other), (1 - odd, to_pair)):
        rows = pl.ds(pl.multiple_of(8 * half, 8), 8)
        for k in range(COMPS):
            fetch(checkpoint.at[k, rows], side.at[pl.ds(8 * k, 8)])
        for axis in range(2):
            fetch(advect.at[axis, rows], side.at[pl.ds(32 + 8 * axis, 8)])
        fetch(diffuse.at[rows], side.at[pl.ds(48, 8)])
    fetch(checkpoint, to_prior.at[pl.ds(0, COMPS)])
    fetch(checkpoint, own_checkpoint)
    fetch(advect, own_advect)
    fetch(diffuse, own_diffuse)
    copies[0].wait()
    for k in range(COMPS):
        spread = jnp.broadcast_to(inverse_row[0:1, k : k + 1], (8, LANES))
        to_prior[COMPS, 0:8, lanes(k)] = spread
        settings[k] = spread
    for copy in copies[1:]:
        copy.wait()


def interior_kernel(checkpoint, advect, diffuse, history, coefs, initial):
    lane = lane_index()
    nothing = jnp.zeros((8, LANES), jnp.float32)
    for g in range(GROUPS):
        for tile in range(2):
            rows = slice(OWN + 8 * tile, OWN + 8 * tile + 8)
            values = coefficient_tiles(advect, diffuse, None, None, tile, g)
            for which in range(5):
                coefs[which, g, rows, :] = values[which]
            for k in range(COMPS):
                value = checkpoint[k, tile * 8 : tile * 8 + 8, lanes(g)]
                initial[k * GROUPS + g, rows, :] = value
        for k in range(COMPS):
            initial[k * GROUPS + g, 0:8, :] = nothing
            initial[k * GROUPS + g, TALL - 8 : TALL, :] = nothing
    for moment in range(STEPS - 1):
        first, tiles = (8, 2) if moment < 3 else (12, 1)
        source = history.at[moment - 1] if moment else initial
        stencil_step(source, history.at[moment], coefs, (0,) * 5, first, tiles, lane)


def forward_kernel(
    pair, other, obs_values, inner, inner_coefs, inner_initial,
    history, coefs, initial, last, observed, arrival,
):
    fetch = pltpu.make_async_copy(obs_values, observed, arrival)
    fetch.start()
    lane = lane_index()
    starts = side_rows()
    for g in range(GROUPS):
        for tile in (2, 3):
            rows = pl.ds(starts[tile - 2], 8)
            values = coefficient_tiles(None, None, pair, other, tile, g)
            for which in range(5):
                coefs[which, g, rows, :] = values[which]
            for k in range(COMPS):
                value = (pair if tile == 2 else other)[8 * k : 8 * k + 8, lanes(g)]
                initial[k * GROUPS + g, rows, :] = value
    for moment in range(STEPS):
        source = history.at[moment - 1] if moment else initial
        for first in (moment + 1, 23 - moment):
            stencil_step(source, history.at[moment], coefs, (0,) * 5, first, 1, lane)
    for cell in range(CELLS):
        last[cell] = history[STEPS - 1, cell, OWN : OWN + 16, :]
    fetch.wait()


def adjoint_kernel(
    obs_rows, weight, advect, diffuse, pair, other, history, following, obs_values,
    own, to_pair, to_other, coefs, work,
):
    lane = lane_index()
    nothing = jnp.zeros((8, LANES), jnp.float32)
    starts = (OWN, OWN + 8) + side_rows()
    for tile in range(4):
        rows = pl.ds(starts[tile], 8)
        groups = [
            coefficient_tiles(advect, diffuse, pair, other, tile, g) for g in range(GROUPS)
        ]
        from_east = eastern([values[2] for values in groups], lane)
        from_west = western([values[1] for values in groups], lane)
        for g in range(GROUPS):
            coefs[0, g, rows, :] = groups[g][0]
            coefs[1, g, rows, :] = from_east[g]
            coefs[2, g, rows, :] = from_west[g]
            coefs[3, g, rows, :] = groups[g][4]
            coefs[4, g, rows, :] = groups[g][3]
    inverses = [following[COMPS, 0:8, lanes(k)] for k in range(COMPS)]
    for g in range(GROUPS):
        for which in (3, 4):
            coefs[which, g, 0:8, :] = nothing
            coefs[which, g, TALL - 8 : TALL, :] = nothing
        for k in range(COMPS):
            cell = k * GROUPS + g
            for slot in range(2):
                for rows in (slice(0, 8), slice(8, 16), slice(32, 40), slice(TALL - 8, TALL)):
                    work[slot, cell, rows, :] = nothing
            for half in range(2):
                start = following[k, 8 * half : 8 * half + 8, lanes(g)]
                end = history[STEPS - 1, cell, OWN + 8 * half : OWN + 8 * half + 8, :]
                work[0, cell, OWN + 8 * half : OWN + 8 * half + 8, :] = inverses[k] * (end - start)
    scale = jnp.broadcast_to(weight[...], (8, LANES))

    for turn in range(STEPS):
        moment = STEPS - 1 - turn
        now = turn % 2
        for entry in range(2):
            offset = pl.multiple_of(obs_rows[entry, moment] * BLOCK, BLOCK)
            there = pl.ds(OWN + offset, 8)
            for k in range(COMPS):
                for g in range(GROUPS):
                    cell = k * GROUPS + g
                    misfit = history[moment, cell, there, :] - obs_values[
                        moment, entry, k, :, lanes(g)
                    ]
                    work[now, cell, there, :] = work[now, cell, there, :] + scale * misfit
        first, tiles = (7 - turn, 3) if turn < 4 else (0, 4)
        stencil_step(
            work.at[now], work.at[1 - now], coefs, (0, 0, 0, 1, -1), first, tiles, lane
        )
    for cell in range(CELLS):
        to_pair[cell] = work[0, cell, pl.ds(starts[2], 8), :]
        to_other[cell] = work[0, cell, pl.ds(starts[3], 8), :]
        own[cell] = work[0, cell, 16:32, :]


def gradient_kernel(settings, own, from_pair, from_other, checkpoint, prior_end, parcels):
    even = jnp.full((8, LANES), lax.axis_index("space_1")) == 0
    squares = jnp.zeros((8, LANES), jnp.float32)
    for k in range(COMPS):
        scale = settings[k]
        for g in range(GROUPS):
            cell = k * GROUPS + g
            pair, other = from_pair[cell], from_other[cell]
            added = (jnp.where(even, other, pair), jnp.where(even, pair, other))
            for half in range(2):
                rows = slice(8 * half, 8 * half + 8)
                forcing = checkpoint[k, rows, lanes(g)] - prior_end[cell, rows, :]
                value = own[cell, rows, :] + added[half] + scale * forcing
                place = 9 * (2 * cell + half)
                parcels[place : place + 8, :] = value
                squares = squares + value * value
    total = jnp.sum(squares, axis=0, keepdims=True)
    for parcel in range(2 * CELLS):
        parcels[9 * parcel + 8 : 9 * parcel + 9, :] = total


def smoothing_kernel(rates, parcels, back, total):
    windows = back.shape[0]
    which = lax.axis_index(TM) // (windows // COMPS)
    running = jnp.zeros((8, LANES), jnp.float32)
    sums = jnp.zeros((1, LANES), jnp.float32)
    for j in range(windows):
        rate = jnp.full((8, LANES), rates[which, j], jnp.float32)
        innovation = jnp.sqrt(1.0 - rate * rate)
        running = rate * running + innovation * parcels[9 * j : 9 * j + 8, :]
        back[j] = innovation * running
        sums = sums + parcels[9 * j + 8 : 9 * j + 9, :]
    total[...] = sums
    running = back[windows - 1]
    for j in range(windows - 2, -1, -1):
        rate = jnp.full((8, LANES), rates[which, j + 1], jnp.float32)
        running = back[j] + rate * running
        back[j] = running


def final_kernel(entries, back, total, direction, rms):
    whole = jnp.broadcast_to(jnp.sum(total[...], axis=1, keepdims=True), (8, LANES))
    rms_tile = jnp.sqrt(whole / entries + 1e-06)
    share = 1.0 / rms_tile
    for k in range(COMPS):
        for g in range(GROUPS):
            for half in range(2):
                direction[k, 8 * half : 8 * half + 8, lanes(g)] = (
                    back[2 * (k * GROUPS + g) + half] * share
                )
    rms[...] = rms_tile[0:1, :]


def on_device(checkpoint, advect, diffuse, obs_rows, obs_values, obs_weight, error_inverse, rates):
    edge_pair, edge_other, start, initial, flow, spread, settings = pl.pallas_call(
        edges_kernel,
        out_shape=(
            local(56, COLUMNS), local(56, COLUMNS), local(COMPS + 1, ROWS, COLUMNS),
            local(COMPS, ROWS, COLUMNS), local(2, ROWS, COLUMNS), local(ROWS, COLUMNS),
            local(COMPS, 8, LANES),
        ),
        in_specs=[FAR] * 4,
        out_specs=(VMEM,) * 7,
        scratch_shapes=[
            pltpu.VMEM((1, COMPS), jnp.float32),
            pltpu.SemaphoreType.DMA((19,)),
        ],
        name="edges",
        compiler_params=GRANT,
    )(
        far(error_inverse), far(checkpoint[0]), far(advect[0]), far(diffuse[0])
    )
    initial, flow, spread, settings = near(initial), near(flow), near(spread), near(settings)
    other = near(crossed(edge_other))
    pair = near(swapped(edge_pair, "space_1"))
    following = near(passed_along(start, TM, -1))
    weight = near(jnp.broadcast_to(obs_weight[None], (1, LANES)))
    sweep_shapes = (
        local(STEPS, CELLS, TALL, LANES), local(5, GROUPS, TALL, LANES), local(CELLS, TALL, LANES)
    )
    inner = pl.pallas_call(
        interior_kernel,
        out_shape=sweep_shapes,
        in_specs=[VMEM] * 3,
        out_specs=(VMEM,) * 3,
        name="interior",
        compiler_params=GRANT,
    )(initial, flow, spread)
    history, _, _, end_state, observed = pl.pallas_call(
        forward_kernel,
        out_shape=sweep_shapes
        + (local(CELLS, ROWS, LANES), local(STEPS, 2, COMPS, BLOCK, COLUMNS)),
        in_specs=[VMEM, VMEM, FAR] + [VMEM] * 3,
        out_specs=(VMEM,) * 5,
        scratch_shapes=[pltpu.SemaphoreType.DMA(())],
        input_output_aliases={3: 0, 4: 1, 5: 2},
        name="forward",
        compiler_params=GRANT,
    )(pair, other, far(obs_values[0]), *(near(value) for value in inner))
    prior_end = near(passed_along(end_state, TM, 1))
    own, to_pair, to_other = pl.pallas_call(
        adjoint_kernel,
        out_shape=(local(CELLS, ROWS, LANES), local(CELLS, 8, LANES), local(CELLS, 8, LANES)),
        in_specs=[SMEM] + [VMEM] * 8,
        out_specs=(VMEM, VMEM, VMEM),
        scratch_shapes=[
            pltpu.VMEM((5, GROUPS, TALL, LANES), jnp.float32),
            pltpu.VMEM((2, CELLS, TALL, LANES), jnp.float32),
        ],
        name="adjoint",
        compiler_params=GRANT,
    )(
        scalars(obs_rows[0].T), weight, flow, spread, pair, other,
        near(history), following, near(observed),
    )
    from_other = near(crossed(to_other))
    from_pair = near(swapped(to_pair, "space_1"))
    windows = lax.axis_size(TM)
    parcels = pl.pallas_call(
        gradient_kernel,
        out_shape=local(9 * 2 * CELLS, LANES),
        in_specs=[VMEM] * 6,
        out_specs=VMEM,
        name="gradient",
        compiler_params=GRANT,
    )(settings, near(own), from_pair, from_other, initial, prior_end)
    arrived = lax.all_to_all(
        parcels.reshape(windows, 1, 9 * LANES), TM, split_axis=0, concat_axis=0, tiled=True
    )
    back, total = pl.pallas_call(
        smoothing_kernel,
        out_shape=(local(windows, 8, LANES), local(1, LANES)),
        in_specs=[SMEM, VMEM],
        out_specs=(VMEM, VMEM),
        name="smoothing",
        compiler_params=GRANT,
    )(scalars(rates.T), near(arrived.reshape(9 * windows, LANES)))
    back = near(lax.all_to_all(back, TM, split_axis=0, concat_axis=0, tiled=True))
    total = total + swapped(total, "space_1")
    total = near(total + swapped(total, "space_0"))
    entries = float(windows * lax.axis_size(SPACE) * checkpoint.size)
    direction, rms = pl.pallas_call(
        lambda *refs: final_kernel(entries, *refs),
        out_shape=(shape(COMPS, ROWS, COLUMNS), shape(1, LANES)),
        in_specs=[VMEM, VMEM],
        out_specs=(VMEM, VMEM),
        name="final",
        compiler_params=GRANT,
    )(back, total)
    return (direction[None], rms[0, 0])


def solution(mesh):
    torus = Mesh(
        mesh.devices.reshape(8, 2, 4, 2, 2), ("tm_0", "tm_1", "tm_2", "space_0", "space_1")
    )

    return jax.shard_map(
        on_device,
        mesh=torus,
        in_specs=(
            P(TM, None, SPACE, None),
            P(TM, None, SPACE, None),
            P(TM, SPACE, None),
            P(TM, None, SPACE),
            P(TM, None, SPACE, None, None, None),
            P(TM),
            P(TM, None),
            P(),
        ),
        out_specs=(P(TM, None, SPACE, None), P()),
        check_vma=False,
    )
```
